512 devices in a mesh: grp: 16 (over x, y_hi), dev: 32 (over y_lo, z, core).
Axes of the slice: x: 4, y: 8 (y_hi: 4, y_lo: 2; y = y_hi * 2 + y_lo), z: 8, core: 2. Of those that a mesh axis runs over, the one named last changes fastest.
Arguments:
- raw: bfloat16 [8192, 16, 4096], P(('grp', 'dev'))
- dark: bfloat16 [16, 4096], replicated, may hold values from 0.049804688 to 0.29882812
- basis: bfloat16 [8, 4096], replicated, may hold values from -3 to 3
- counts: int32 [8192], P(('grp', 'dev')), may hold values from 1 to 16, as said below
- positions: int32 [8192], replicated, may hold values from 0 to 8191, as said below
Outputs:
- corrected: bfloat16 [8192, 16, 4096], P(('grp', 'dev'))
- pooled: bfloat16 [16, 16, 1, 491520], P('grp', None, None, 'dev')
The draws below stay inside these ranges and needn't reach their ends.
Inputs may be any that keep to these rules, and one draw needn't show every extreme that they name: `counts`: the first tile of every device (16 tiles in acquisition order) has all 16 planes. A permutation of the tile positions of the slide image. The 16 tiles of the device at grp index g and dev index d lie in 16 different bands, all at tile columns d * 16 to d * 16 + 15.
All inputs are finite; a program needn't handle non-finite values.
Results may differ from the reference program's by a relative error of at most 0.0046.
Values may be sent and summed in bfloat16 or wider, within the bound.
No kernel may reach another device: no remote copies, remote signals or barrier semaphores. Data moves between devices by JAX's collectives and lax.ppermute only.
A program may use at most 128 MiB of HBM per device.

```python
import jax
import jax.numpy as jnp
from jax import lax

ROWS = 2
COLS = 2048
OVL = 128
PLANES = 16
RANK = 8
TILES_DEV = 16
TILES = 8192
PIX = 4096
BAND = 512
N_GRP = 16
N_DEV = 32


def shading_parts(key):
    basis_key = jax.random.fold_in(key, 11)
    basis = jnp.clip(jax.random.normal(basis_key, (RANK, PIX), jnp.float32), -3.0, 3.0)
    weights = jax.random.normal(jax.random.fold_in(key, 12), (RANK, PLANES), jnp.float32) * 0.1
    drift = jax.random.normal(jax.random.fold_in(key, 13), (RANK, PLANES), jnp.float32) * 0.15
    blocks = TILES // TILES_DEV
    offsets = jax.random.normal(jax.random.fold_in(key, 14), (blocks, RANK, PLANES), jnp.float32) * 0.3
    return (basis, weights, drift, offsets)


def draw_basis(key, part):
    basis, weights, drift, offsets = shading_parts(key)
    return basis.astype(jnp.bfloat16)


def draw_raw(key, part):
    basis, weights, drift, offsets = shading_parts(key)
    blocks = TILES // TILES_DEV
    order = jnp.arange(TILES, dtype=jnp.float32) / TILES
    block_of = jnp.arange(TILES, dtype=jnp.int32) // TILES_DEV
    tile_weights = weights[None] + order[:, None, None] * drift[None] + offsets[block_of]
    shade = jnp.einsum('tkp,kx->tpx', tile_weights, basis)
    block_bright = jnp.exp(jax.random.uniform(jax.random.fold_in(key, 23), (blocks,), jnp.float32, jnp.log(0.3), jnp.log(3.0)))
    rough = jax.random.uniform(jax.random.fold_in(key, 22), (TILES, PLANES, PIX), jnp.float32, 0.5, 1.5)
    bright = 0.4 * jnp.exp(jnp.log(3.0) * order) * jax.random.uniform(jax.random.fold_in(key, 21), (TILES,), jnp.float32, 0.7, 1.4)
    bright = bright * block_bright[block_of]
    values = 0.36 + bright[:, None, None] * rough * jnp.exp(shade)
    return values.astype(jnp.bfloat16)


def draw_counts(key, part):
    drawn = jax.random.randint(jax.random.fold_in(key, 31), (TILES,), 1, PLANES + 1)
    first = jnp.arange(TILES, dtype=jnp.int32) % TILES_DEV == 0
    return jnp.where(first, PLANES, drawn).astype(jnp.int32)


def draw_positions(key, part):
    sources = N_GRP * N_DEV
    band_keys = jax.random.split(jax.random.fold_in(key, 41), sources)
    bands = jax.vmap(lambda k: jax.random.permutation(k, N_GRP))(band_keys).reshape(N_GRP, N_DEV, TILES_DEV)
    slot_keys = jax.random.split(jax.random.fold_in(key, 42), sources)
    slots = jax.vmap(lambda k: jax.random.permutation(k, N_GRP))(slot_keys).reshape(N_GRP, N_DEV, N_GRP)
    column_ids = jnp.arange(N_DEV, dtype=jnp.int32)[None, :, None]
    source_ids = jnp.arange(N_GRP, dtype=jnp.int32)[:, None, None]
    slot = slots[bands, column_ids, source_ids]
    places = bands * BAND + column_ids * TILES_DEV + slot
    return places.reshape(TILES).astype(jnp.int32)


def setup_inputs(seed: int = 0) -> dict:
    key_list = jax.random.split(jax.random.key(seed), 6)
    raw = draw_raw(jax.random.fold_in(key_list[5], 71), 0)
    dark = jnp.clip(jax.random.uniform(key_list[1], (PLANES, PIX), jnp.float32, 0.049804688, 0.29882812), 0.049804688, 0.29882812).astype(jnp.bfloat16)
    basis = draw_basis(jax.random.fold_in(key_list[5], 71), 0)
    counts = draw_counts(jax.random.fold_in(key_list[5], 71), 0)
    positions = draw_positions(jax.random.fold_in(key_list[5], 71), 0)
    return {"raw": raw, "dark": dark, "basis": basis, "counts": counts, "positions": positions}


def feather():
    column = jnp.arange(COLS, dtype=jnp.float32) + 0.5
    return jnp.minimum(1.0, jnp.minimum(column / OVL, (COLS - column) / OVL))


def pooling(tiles):
    count = tiles.shape[0]
    shaped = tiles.reshape(count, PLANES, ROWS, COLS) * feather()
    return jnp.sum(shaped.reshape(count, PLANES, ROWS // 2, 2, COLS // 2, 2), axis=(3, 5)) * 0.25


def reference(raw, dark, basis, counts, positions):
    live = (jnp.arange(PLANES, dtype=jnp.int32)[None, :] < counts[:, None]).astype(jnp.float32)
    blocks = TILES // TILES_DEV
    raw_blocks = raw.reshape(blocks, TILES_DEV, PLANES, PIX)
    live_blocks = live.reshape(blocks, TILES_DEV, PLANES)
    basis_f = basis.astype(jnp.float32)
    dark_f = dark.astype(jnp.float32)

    def gather_terms(carry, item):
        tiles, alive = item
        tiles_f = tiles.astype(jnp.float32)
        projected = jnp.einsum("kx,tpx->tkp", basis_f, tiles_f)
        local_proj = jnp.sum(projected * alive[:, None, :], axis=0)
        local_sum = jnp.sum(jnp.sum(tiles_f, axis=2) * alive, axis=0)
        return (carry[0] + local_proj, carry[1] + local_sum, carry[2] + jnp.sum(alive, axis=0)), None

    start = (jnp.zeros((RANK, PLANES), jnp.float32), jnp.zeros((PLANES,), jnp.float32), jnp.zeros((PLANES,), jnp.float32))
    (proj, total, alive), _ = lax.scan(gather_terms, start, (raw_blocks, live_blocks))
    dark_proj = jnp.dot(basis, dark.T, preferred_element_type=jnp.float32)
    dark_sum = jnp.sum(dark_f, axis=1)
    coef = (proj - alive[None, :] * dark_proj) / (total - alive * dark_sum)[None, :]
    shade = jnp.dot(coef.T, basis_f, precision=lax.Precision.HIGHEST)
    inverse = jnp.exp(-shade)

    def repair(item):
        tiles, alive_rows = item
        return ((tiles.astype(jnp.float32) - dark_f[None]) * inverse[None] * alive_rows[:, :, None]).astype(jnp.bfloat16)

    corrected = lax.map(repair, (raw_blocks, live_blocks)).reshape(TILES, PLANES, PIX)
    order = jnp.argsort(positions).astype(jnp.int32)
    half_step = (COLS - OVL) // 2
    half_ovl = OVL // 2

    def band_rows(band):
        chosen = lax.dynamic_slice_in_dim(order, band * BAND, BAND)
        cells = pooling(corrected[chosen].astype(jnp.float32)).astype(jnp.bfloat16)
        cells = lax.optimization_barrier(cells)
        head = cells[..., :half_step].astype(jnp.float32)
        tail = cells[..., half_step:]
        carried = jnp.concatenate([jnp.zeros_like(tail[:1]), tail[:-1]], axis=0)
        carried = jnp.pad(carried, ((0, 0), (0, 0), (0, 0), (0, half_step - half_ovl))).astype(jnp.float32)
        merged = head + carried
        return jnp.transpose(merged, (1, 2, 0, 3)).reshape(PLANES, ROWS // 2, BAND * half_step).astype(jnp.bfloat16)

    pooled = lax.map(band_rows, jnp.arange(N_GRP, dtype=jnp.int32))
    return corrected, pooled
```

```python
import jax
import jax.numpy as jnp
from jax import lax
from jax.experimental import pallas as pl
from jax.experimental.pallas import tpu as pltpu
from jax.sharding import Mesh
from jax.sharding import PartitionSpec as P

ROWS = 2
COLS = 2048
OVL = 128
GRP = ("grp_0", "grp_1")
DEV = ("dev_0", "dev_1", "dev_2")
GRP_DEV = GRP + DEV
FIRST = ("dev_1", "dev_2")
SECOND = ("grp_0", "grp_1", "dev_0")
LANES = 128
WIDE = 256
HALF = LANES // 2


def terms_kernel(counts, raw, dark, basis, out):
    tiles, planes, pixels = raw.shape
    rank = basis.shape[0]
    ones = jnp.ones((rank, pixels), jnp.bfloat16)
    weights = jnp.concatenate([basis[...], ones], axis=0)
    contract = (((1,), (1,)), ((), ()))
    rows = lax.dot_general(
        raw[...].reshape(tiles * planes, pixels), weights, contract,
        preferred_element_type=jnp.float32,
    ).reshape(tiles, planes, 2 * rank)
    dark_rows = lax.dot_general(
        dark[...], weights, contract, preferred_element_type=jnp.float32
    )
    plane = lax.broadcasted_iota(jnp.int32, (planes, 2 * rank), 0)
    acc = jnp.zeros((planes, 2 * rank), jnp.float32)
    for t in range(tiles):
        acc = acc + jnp.where(plane < counts[t], rows[t] - dark_rows, 0.0)
    half = planes // 2
    pad = jnp.zeros((half, HALF - 2 * rank), jnp.float32)
    out[...] = jnp.concatenate([acc[:half], pad, acc[half:], pad], axis=1)


def pair_weights():
    row = lax.broadcasted_iota(jnp.int32, (WIDE, LANES), 0)
    col = lax.broadcasted_iota(jnp.int32, (WIDE, LANES), 1)
    hit = row // 2 == col
    up = (row.astype(jnp.float32) + 0.5) / OVL
    down = (WIDE - row.astype(jnp.float32) - 0.5) / OVL
    def of(scale):
        return jnp.where(hit, 0.25 * jnp.minimum(1.0, scale), 0.0).astype(jnp.bfloat16)
    return of(up), of(jnp.ones_like(up)), of(down)


def correct_kernel(counts, bands, parts, raw, dark, basis, corrected, cells, coef3, stage, sem):
    tiles, planes, pixels = raw.shape
    rank = basis.shape[0]
    half = planes // 2
    total = jnp.sum(parts[...], axis=0)
    terms = jnp.concatenate([total[:, :HALF], total[:, HALF:]], axis=0)
    coef = terms[:, :rank] / terms[:, rank : rank + 1]
    high = coef.astype(jnp.bfloat16)
    rest = coef - high.astype(jnp.float32)
    middle = rest.astype(jnp.bfloat16)
    low = (rest - middle.astype(jnp.float32)).astype(jnp.bfloat16)
    coef3[...] = jnp.concatenate([high, middle, low], axis=1)
    plane = lax.broadcasted_iota(jnp.int32, (planes, WIDE), 0)
    first, inner, last = pair_weights()
    blocks = COLS // WIDE
    copies = []
    for j in range(blocks):
        weight = first if j == 0 else last if j == blocks - 1 else inner
        acc = None
        for r in range(ROWS):
            x = slice(r * COLS + j * WIDE, r * COLS + (j + 1) * WIDE)
            base = basis[:, x]
            shade = jnp.dot(
                coef3[...], jnp.concatenate([base, base, base], axis=0),
                preferred_element_type=jnp.float32,
            )
            inverse = jnp.exp(-shade)
            dark_f = dark[:, x].astype(jnp.float32)
            for t in range(tiles):
                value = (raw[t, :, x].astype(jnp.float32) - dark_f) * inverse
                stage[t, :, x] = jnp.where(plane < counts[t], value, 0.0).astype(jnp.bfloat16)
            copy = pltpu.make_async_copy(
                stage.at[:, :, x], corrected.at[:, :, x], sem.at[j * ROWS + r]
            )
            copy.start()
            copies.append(copy)
            part = jnp.dot(
                stage[:, :, x].reshape(tiles * planes, WIDE), weight,
                preferred_element_type=jnp.float32,
            )
            acc = part if acc is None else acc + part
        pooled = acc.astype(jnp.bfloat16).reshape(tiles, planes, LANES)
        for t in range(tiles):
            cells[bands[t], :, j * LANES : (j + 1) * LANES] = pooled[t]
    for copy in copies:
        copy.wait()


def stitch_kernel(sources, arrived, spill, out):
    count, planes, width = arrived.shape
    step = (COLS - OVL) // 2
    lane = lax.broadcasted_iota(jnp.int32, (planes, LANES), 1)
    left = lane < HALF
    carry = jnp.where(left, pltpu.roll(spill[...].astype(jnp.float32), HALF, 1), 0.0)
    for j in range(0, count, 2):
        here = arrived[sources[j]].astype(jnp.float32)
        after = pltpu.roll(arrived[sources[j + 1]].astype(jnp.float32), HALF, 1)
        edge = after[:, :LANES]
        segment = jnp.concatenate(
            [
                here[:, :LANES] + carry,
                here[:, LANES : width - LANES],
                here[:, width - LANES :] + jnp.where(left, 0.0, edge),
                after[:, LANES:],
            ],
            axis=1,
        )
        out[:, j * step : (j + 2) * step] = segment.astype(jnp.bfloat16)
        carry = jnp.where(left, edge, 0.0)


SMEM = pl.BlockSpec(memory_space=pltpu.SMEM)
VMEM = pl.BlockSpec(memory_space=pltpu.VMEM)
ANY = pl.BlockSpec(memory_space=pl.ANY)


def summed_exchange(value, axes):
    copies = jnp.broadcast_to(value[None], (lax.axis_size(axes), *value.shape))
    return lax.all_to_all(copies, axes, split_axis=0, concat_axis=0, tiled=True)


def per_device(raw, dark, basis, counts, positions):
    tiles, planes, pixels = raw.shape
    groups = lax.axis_size(GRP)
    columns = lax.axis_size(DEV)
    band_size = columns * tiles
    width = COLS // 2
    terms = pl.pallas_call(
        terms_kernel,
        out_shape=jax.ShapeDtypeStruct((planes // 2, LANES), jnp.float32),
        in_specs=[SMEM, VMEM, VMEM, VMEM],
        out_specs=VMEM,
        name="terms",
    )(counts, raw, dark, basis)
    here_grp = lax.axis_index(GRP)
    here_dev = lax.axis_index(DEV)
    layout = positions.reshape(groups, columns, tiles)
    column_tiles = lax.dynamic_index_in_dim(layout, here_dev, 1, False)
    mine = lax.dynamic_index_in_dim(column_tiles, here_grp, 0, False)
    bands = mine // band_size
    arrives = column_tiles // band_size == here_grp
    slot_of = jnp.sum(jnp.where(arrives, column_tiles % tiles, 0), axis=1)
    slots = jnp.arange(tiles, dtype=jnp.int32)
    ids = jnp.arange(groups, dtype=jnp.int32)
    sources = jnp.sum(jnp.where(slot_of[None, :] == slots[:, None], ids[None, :], 0), axis=1)

    once = jnp.sum(summed_exchange(terms, FIRST), axis=0)
    parts = summed_exchange(once, SECOND)
    corrected, outgoing = pl.pallas_call(
        correct_kernel,
        out_shape=(
            jax.ShapeDtypeStruct(raw.shape, jnp.bfloat16),
            jax.ShapeDtypeStruct((groups, planes, width), jnp.bfloat16),
        ),
        in_specs=[SMEM, SMEM, VMEM, VMEM, VMEM, VMEM],
        out_specs=(ANY, VMEM),
        scratch_shapes=[
            pltpu.VMEM((planes, 3 * basis.shape[0]), jnp.bfloat16),
            pltpu.VMEM(raw.shape, jnp.bfloat16),
            pltpu.SemaphoreType.DMA((pixels // WIDE,)),
        ],
        name="correct",
    )(counts, bands, parts, raw, dark, basis)
    arrived = lax.all_to_all(outgoing, GRP, split_axis=0, concat_axis=0, tiled=True)
    tail = lax.dynamic_slice(
        arrived, (sources[tiles - 1], 0, width - LANES), (1, planes, LANES)
    )[0]
    spill = lax.ppermute(tail, DEV, [(d, d + 1) for d in range(columns - 1)])
    pooled = pl.pallas_call(
        stitch_kernel,
        out_shape=jax.ShapeDtypeStruct((planes, tiles * (COLS - OVL) // 2), jnp.bfloat16),
        in_specs=[SMEM, VMEM, VMEM],
        out_specs=VMEM,
        name="stitch",
    )(sources, arrived, spill)
    return corrected, pooled.reshape(1, planes, ROWS // 2, tiles * (COLS - OVL) // 2)


def solution(mesh):
    split = Mesh(mesh.devices.reshape(4, 4, 2, 8, 2), GRP_DEV)
    placed = (P(GRP_DEV, None, None), P(), P(), P(GRP_DEV), P())
    return jax.shard_map(
        per_device,
        mesh=split,
        in_specs=placed,
        out_specs=(P(GRP_DEV, None, None), P(GRP, None, None, DEV)),
        check_vma=False,
    )
```

```python
import jax
import jax.numpy as jnp
from jax import lax
from jax.experimental import pallas as pl
from jax.experimental.pallas import tpu as pltpu
from jax.sharding import Mesh
from jax.sharding import PartitionSpec as P

ROWS = 2
COLS = 2048
OVL = 128
GRP = ("grp_0", "grp_1")
DEV = ("dev_0", "dev_1", "dev_2")
GRP_DEV = GRP + DEV
FIRST = ("dev_1", "dev_2")
SECOND = ("grp_0", "grp_1", "dev_0")
LANES = 128
WIDE = 256
HALF = LANES // 2
SUBLANES = 8
PARTS = 16
CHUNKS = 4


def packed(rows):
    planes = rows.shape[0]
    lane = lax.broadcasted_iota(jnp.int32, (planes, LANES), 1)
    plane = lax.broadcasted_iota(jnp.int32, (planes, LANES), 0)
    wide = jnp.where(lane < PARTS, rows, 0.0)
    for shift in (PARTS, 2 * PARTS, 4 * PARTS):
        wide = wide + pltpu.roll(wide, shift, 1)
    chosen = jnp.where(lane // PARTS == plane % SUBLANES, wide, 0.0)
    return jnp.sum(chosen.reshape(planes // SUBLANES, SUBLANES, LANES), axis=1)


def unpacked(rows):
    count = rows.shape[0]
    planes = count * SUBLANES
    lane = lax.broadcasted_iota(jnp.int32, (planes, LANES), 1)
    plane = lax.broadcasted_iota(jnp.int32, (planes, LANES), 0)
    spread = jnp.broadcast_to(rows[:, None, :], (count, SUBLANES, LANES)).reshape(planes, LANES)
    wide = jnp.where(lane // PARTS == plane % SUBLANES, spread, 0.0)
    for shift in (PARTS, 2 * PARTS, 4 * PARTS):
        wide = wide + pltpu.roll(wide, shift, 1)
    return wide


def terms_kernel(
    counts_h, raw_h, dark_h, basis_h, out, raw, dark, basis, edges, counts, sem
):
    tiles, planes, pixels = raw.shape
    rank = basis.shape[0]
    chunk = tiles // CHUNKS
    small = [
        pltpu.make_async_copy(basis_h, basis, sem.at[CHUNKS]),
        pltpu.make_async_copy(dark_h, dark, sem.at[CHUNKS + 1]),
        pltpu.make_async_copy(counts_h, counts, sem.at[CHUNKS + 2]),
    ]
    large = []
    for c in range(CHUNKS):
        t = slice(c * chunk, (c + 1) * chunk)
        large.append(pltpu.make_async_copy(raw_h.at[t], raw.at[t], sem.at[c]))
    for copy in small + large:
        copy.start()
    for copy in small:
        copy.wait()
    weights = jnp.concatenate([basis[...], jnp.ones((rank, pixels), jnp.bfloat16)], axis=0)
    contract = (((1,), (1,)), ((), ()))
    dark_rows = lax.dot_general(
        dark[...], weights, contract, preferred_element_type=jnp.float32
    )
    plane = lax.broadcasted_iota(jnp.int32, (planes, 2 * rank), 0)
    wide_plane = lax.broadcasted_iota(jnp.int32, (planes, OVL), 0)
    acc = jnp.zeros((planes, 2 * rank), jnp.float32)
    ends = [slice((r + 1) * COLS - OVL, (r + 1) * COLS) for r in range(ROWS)]
    dark_ends = [dark[:, x].astype(jnp.float32) for x in ends]
    for c in range(CHUNKS):
        large[c].wait()
        t0 = c * chunk
        rows = lax.dot_general(
            raw[t0 : t0 + chunk].reshape(chunk * planes, pixels), weights, contract,
            preferred_element_type=jnp.float32,
        ).reshape(chunk, planes, 2 * rank)
        for i in range(chunk):
            t = t0 + i
            acc = acc + jnp.where(plane < counts[t], rows[i] - dark_rows, 0.0)
            for r in range(ROWS):
                value = raw[t, :, ends[r]].astype(jnp.float32)
                kept = jnp.where(wide_plane < counts[t], value, dark_ends[r])
                edges[t, :, r * OVL : (r + 1) * OVL] = kept.astype(jnp.bfloat16)
    pad = jnp.zeros((planes, LANES - 2 * rank), jnp.float32)
    rows = packed(jnp.concatenate([acc, pad], axis=1))
    out[...] = jnp.broadcast_to(rows[None], out.shape)


def pair_weights():
    row = lax.broadcasted_iota(jnp.int32, (WIDE, LANES), 0)
    col = lax.broadcasted_iota(jnp.int32, (WIDE, LANES), 1)
    hit = row // 2 == col
    up = (row.astype(jnp.float32) + 0.5) / OVL
    down = (WIDE - row.astype(jnp.float32) - 0.5) / OVL
    def of(scale):
        return jnp.where(hit, 0.25 * jnp.minimum(1.0, scale), 0.0).astype(jnp.bfloat16)
    return of(up), of(jnp.ones_like(up)), of(down)


def tail_weights():
    row = lax.broadcasted_iota(jnp.int32, (ROWS * OVL, LANES), 0) % OVL
    col = lax.broadcasted_iota(jnp.int32, (ROWS * OVL, LANES), 1) % HALF
    scale = jnp.minimum(1.0, (OVL - row.astype(jnp.float32) - 0.5) / OVL)
    return jnp.where(row // 2 == col, 0.25 * scale, 0.0).astype(jnp.bfloat16)


def correct_kernel(
    counts_h, positions_h, parts, raw, dark, basis, edges, corrected_h, cells_h,
    corrected, cells, inverse, counts, positions, sem,
):
    tiles, planes, pixels = raw.shape
    rank = basis.shape[0]
    half = planes // 2
    copies = [
        pltpu.make_async_copy(counts_h, counts, sem.at[0]),
        pltpu.make_async_copy(positions_h, positions, sem.at[1]),
    ]
    for copy in copies:
        copy.start()
    columns = lax.axis_size(DEV)
    own = (lax.axis_index(GRP) * columns + lax.axis_index(DEV)) * tiles
    before = jnp.maximum(own - tiles, 0)
    terms = unpacked(jnp.sum(parts[...], axis=0))
    coef = (terms / pltpu.roll(terms, LANES - rank, 1))[:, :rank]
    high = coef.astype(jnp.bfloat16)
    rest = coef - high.astype(jnp.float32)
    middle = rest.astype(jnp.bfloat16)
    low = (rest - middle.astype(jnp.float32)).astype(jnp.bfloat16)
    coef3 = jnp.concatenate([high, middle, low], axis=1)
    base = basis[...]
    shade = jnp.dot(
        coef3, jnp.concatenate([base, base, base], axis=0), preferred_element_type=jnp.float32
    )
    inverse[...] = jnp.exp(-shade)
    leaving = []

    def leave(source, target):
        copy = pltpu.make_async_copy(source, target, sem.at[2 + len(leaving)])
        copy.start()
        leaving.append(copy)

    ends = [slice((r + 1) * COLS - OVL, (r + 1) * COLS) for r in range(ROWS)]
    value = jnp.concatenate(
        [
            ((edges[:, :, r * OVL : (r + 1) * OVL].astype(jnp.float32)
              - dark[:, x].astype(jnp.float32)[None]) * inverse[:, x][None]).astype(jnp.bfloat16)
            for r, x in enumerate(ends)
        ],
        axis=2,
    )
    tails = jnp.dot(
        value.reshape(tiles * planes, ROWS * OVL), tail_weights(),
        preferred_element_type=jnp.float32,
    ).reshape(tiles, planes, LANES)
    left = lax.broadcasted_iota(jnp.int32, (half, LANES), 1) < HALF
    for copy in copies:
        copy.wait()
    for t in range(tiles):
        band = positions[before + t] // (columns * tiles)
        joined = jnp.where(left, tails[t, :half], tails[t, half:])
        cells[band, COLS // WIDE * planes :, :] = joined.astype(jnp.bfloat16)
    plane = lax.broadcasted_iota(jnp.int32, (planes, WIDE), 0)
    first, inner, last = pair_weights()
    blocks = COLS // WIDE
    for j in range(blocks):
        weight = first if j == 0 else last if j == blocks - 1 else inner
        acc = None
        for r in range(ROWS):
            x = slice(r * COLS + j * WIDE, r * COLS + (j + 1) * WIDE)
            scale = inverse[:, x]
            dark_f = dark[:, x].astype(jnp.float32)
            for t in range(tiles):
                value = (raw[t, :, x].astype(jnp.float32) - dark_f) * scale
                corrected[t, :, x] = jnp.where(plane < counts[t], value, 0.0).astype(jnp.bfloat16)
            leave(corrected.at[:, :, x], corrected_h.at[:, :, x])
            part = jnp.dot(
                corrected[:, :, x].reshape(tiles * planes, WIDE), weight,
                preferred_element_type=jnp.float32,
            )
            acc = part if acc is None else acc + part
        pooled = acc.astype(jnp.bfloat16).reshape(tiles, planes, LANES)
        for t in range(tiles):
            band = positions[own + t] // (columns * tiles)
            cells[band, j * planes : (j + 1) * planes, :] = pooled[t]
        x = slice(j * planes, (j + 1) * planes + (half if j == blocks - 1 else 0))
        leave(cells.at[:, x, :], cells_h.at[:, x, :])
    for copy in leaving:
        copy.wait()


def stitch_kernel(sources, arrived, out_h, out, sem):
    planes = out.shape[0]
    count = arrived.shape[0]
    half = planes // 2
    blocks = COLS // 2 // LANES
    step = (COLS - OVL) // 2
    lane = lax.broadcasted_iota(jnp.int32, (planes, LANES), 1)
    left = lane < HALF

    def tile(source):
        return jnp.concatenate(
            [arrived[source, j * planes : (j + 1) * planes, :] for j in range(blocks)], axis=1
        ).astype(jnp.float32)

    spill = arrived[sources[count], blocks * planes :, :].astype(jnp.float32)
    spill = jnp.concatenate([spill, pltpu.roll(spill, HALF, 1)], axis=0)
    carry = jnp.where(left & (lax.axis_index(DEV) > 0), spill, 0.0)
    copies = []
    for j in range(0, count, 2):
        here = tile(sources[j])
        after = pltpu.roll(tile(sources[j + 1]), HALF, 1)
        edge = after[:, :LANES]
        width = here.shape[1]
        segment = jnp.concatenate(
            [
                here[:, :LANES] + carry,
                here[:, LANES : width - LANES],
                here[:, width - LANES :] + jnp.where(left, 0.0, edge),
                after[:, LANES:],
            ],
            axis=1,
        )
        x = slice(j * step, (j + 2) * step)
        out[:, x] = segment.astype(jnp.bfloat16)
        copy = pltpu.make_async_copy(out.at[:, x], out_h.at[:, x], sem.at[j // 2])
        copy.start()
        copies.append(copy)
        carry = jnp.where(left, edge, 0.0)
    for copy in copies:
        copy.wait()


SMEM = pl.BlockSpec(memory_space=pltpu.SMEM)
VMEM = pl.BlockSpec(memory_space=pltpu.VMEM)
HBM = pl.BlockSpec(memory_space=pltpu.HBM)
LIMIT = pltpu.CompilerParams(vmem_limit_bytes=16 << 20)


def in_vmem(value):
    return pltpu.with_memory_space_constraint(value, pltpu.VMEM)


def in_hbm(value):
    return pltpu.with_memory_space_constraint(value, pltpu.HBM)


def exchanged(copies, axes):
    return lax.all_to_all(copies, axes, split_axis=0, concat_axis=0, tiled=True)


def sources_of(positions, column, groups, columns, tiles):
    layout = positions.reshape(groups, columns, tiles)
    column_tiles = lax.dynamic_index_in_dim(layout, column, 1, False)
    arrives = column_tiles // (columns * tiles) == lax.axis_index(GRP)
    slot_of = jnp.sum(jnp.where(arrives, column_tiles % tiles, 0), axis=1)
    slots = jnp.arange(tiles, dtype=jnp.int32)
    ids = jnp.arange(groups, dtype=jnp.int32)
    return jnp.sum(jnp.where(slot_of[None, :] == slots[:, None], ids[None, :], 0), axis=1)


def per_device(raw, dark, basis, counts, positions):
    tiles, planes, pixels = raw.shape
    groups = lax.axis_size(GRP)
    columns = lax.axis_size(DEV)
    width = COLS // 2
    span = tiles * (COLS - OVL) // 2
    height = width // LANES * planes + planes // 2
    first, second = lax.axis_size(FIRST), lax.axis_size(SECOND)
    terms, raw_v, dark_v, basis_v, edges = pl.pallas_call(
        terms_kernel,
        out_shape=(
            pltpu.VMEM((first, planes // SUBLANES, LANES), jnp.float32),
            pltpu.VMEM(raw.shape, jnp.bfloat16),
            pltpu.VMEM(dark.shape, jnp.bfloat16),
            pltpu.VMEM(basis.shape, jnp.bfloat16),
            jax.ShapeDtypeStruct((tiles, planes, ROWS * OVL), jnp.bfloat16),
        ),
        in_specs=[HBM, HBM, HBM, HBM],
        out_specs=(VMEM, VMEM, VMEM, VMEM, VMEM),
        scratch_shapes=[
            pltpu.SMEM((tiles,), jnp.int32),
            pltpu.SemaphoreType.DMA((CHUNKS + 3,)),
        ],
        compiler_params=LIMIT,
        name="terms",
    )(in_hbm(counts), in_hbm(raw), in_hbm(dark), in_hbm(basis))
    once = jnp.sum(exchanged(terms, FIRST), axis=0)
    edges, positions_late, once = lax.optimization_barrier((edges, positions, once))
    parts = exchanged(jnp.broadcast_to(once[None], (second, *once.shape)), SECOND)
    edges = lax.ppermute(edges, DEV, [(d, d + 1) for d in range(columns - 1)])
    here_dev = lax.axis_index(DEV)
    own_sources = sources_of(positions_late, here_dev, groups, columns, tiles)
    left_dev = jnp.maximum(here_dev - 1, 0)
    left_sources = sources_of(positions_late, left_dev, groups, columns, tiles)
    sources = jnp.concatenate([own_sources, left_sources[tiles - 1 :]])
    corrected, outgoing = pl.pallas_call(
        correct_kernel,
        out_shape=(
            jax.ShapeDtypeStruct(raw.shape, jnp.bfloat16),
            jax.ShapeDtypeStruct((groups, height, LANES), jnp.bfloat16),
        ),
        in_specs=[HBM, HBM, VMEM, VMEM, VMEM, VMEM, VMEM],
        out_specs=(HBM, HBM),
        scratch_shapes=[
            pltpu.VMEM(raw.shape, jnp.bfloat16),
            pltpu.VMEM((groups, height, LANES), jnp.bfloat16),
            pltpu.VMEM(dark.shape, jnp.float32),
            pltpu.SMEM((tiles,), jnp.int32),
            pltpu.SMEM(positions.shape, jnp.int32),
            pltpu.SemaphoreType.DMA((2 + pixels // WIDE + width // LANES,)),
        ],
        compiler_params=LIMIT,
        name="correct",
    )(
        in_hbm(counts), in_hbm(positions), in_vmem(parts), in_vmem(raw_v), in_vmem(dark_v),
        in_vmem(basis_v), in_vmem(edges),
    )
    arrived = exchanged(outgoing, GRP)
    pooled = pl.pallas_call(
        stitch_kernel,
        out_shape=jax.ShapeDtypeStruct((planes, span), jnp.bfloat16),
        in_specs=[SMEM, VMEM],
        out_specs=HBM,
        scratch_shapes=[
            pltpu.VMEM((planes, span), jnp.bfloat16),
            pltpu.SemaphoreType.DMA((tiles // 2,)),
        ],
        compiler_params=LIMIT,
        name="stitch",
    )(sources, in_vmem(arrived))
    return corrected, pooled.reshape(1, planes, ROWS // 2, span)


def solution(mesh):
    split = Mesh(mesh.devices.reshape(4, 4, 2, 8, 2), GRP_DEV)
    placed = (P(GRP_DEV, None, None), P(), P(), P(GRP_DEV), P())
    return jax.shard_map(
        per_device,
        mesh=split,
        in_specs=placed,
        out_specs=(P(GRP_DEV, None, None), P(GRP, None, None, DEV)),
        check_vma=False,
    )
```

```python
import jax
import jax.numpy as jnp
from jax import lax
from jax.experimental import pallas as pl
from jax.experimental.pallas import tpu as pltpu
from jax.sharding import Mesh
from jax.sharding import PartitionSpec as P

ROWS = 2
COLS = 2048
OVL = 128
GRP = ("grp_0", "grp_1")
DEV = ("dev_0", "dev_1", "dev_2")
GRP_DEV = GRP + DEV
FIRST = ("dev_1", "dev_2")
SECOND = ("grp_0", "grp_1", "dev_0")
LANES = 128
WIDE = 256
HALF = LANES // 2
SUBLANES = 8
PARTS = 16
CHUNKS = 4
EARLY = 3


def packed(rows):
    planes = rows.shape[0]
    lane = lax.broadcasted_iota(jnp.int32, (planes, LANES), 1)
    plane = lax.broadcasted_iota(jnp.int32, (planes, LANES), 0)
    wide = jnp.where(lane < PARTS, rows, 0.0)
    for shift in (PARTS, 2 * PARTS, 4 * PARTS):
        wide = wide + pltpu.roll(wide, shift, 1)
    chosen = jnp.where(lane // PARTS == plane % SUBLANES, wide, 0.0)
    return jnp.sum(chosen.reshape(planes // SUBLANES, SUBLANES, LANES), axis=1)


def unpacked(rows):
    count = rows.shape[0]
    planes = count * SUBLANES
    lane = lax.broadcasted_iota(jnp.int32, (planes, LANES), 1)
    plane = lax.broadcasted_iota(jnp.int32, (planes, LANES), 0)
    spread = jnp.broadcast_to(rows[:, None, :], (count, SUBLANES, LANES)).reshape(planes, LANES)
    wide = jnp.where(lane // PARTS == plane % SUBLANES, spread, 0.0)
    for shift in (PARTS, 2 * PARTS, 4 * PARTS):
        wide = wide + pltpu.roll(wide, shift, 1)
    return wide


def terms_kernel(
    counts_h, raw_h, dark_h, basis_h, out, raw, dark, basis, edges, limits, counts, sem
):
    tiles, planes, pixels = raw.shape
    rank = basis.shape[0]
    chunk = tiles // CHUNKS
    small = [
        pltpu.make_async_copy(counts_h, counts, sem.at[CHUNKS]),
        pltpu.make_async_copy(basis_h, basis, sem.at[CHUNKS + 1]),
        pltpu.make_async_copy(dark_h, dark, sem.at[CHUNKS + 2]),
    ]
    large = []
    for c in range(CHUNKS):
        t = slice(c * chunk, (c + 1) * chunk)
        large.append(pltpu.make_async_copy(raw_h.at[t], raw.at[t], sem.at[c]))
    for copy in small + large:
        copy.start()
    small[1].wait()
    weights = jnp.concatenate([basis[...], jnp.ones((rank, pixels), jnp.bfloat16)], axis=0)
    contract = (((1,), (1,)), ((), ()))
    small[2].wait()
    dark_rows = lax.dot_general(
        dark[...], weights, contract, preferred_element_type=jnp.float32
    )
    plane = lax.broadcasted_iota(jnp.int32, (planes, 2 * rank), 0)
    wide_plane = lax.broadcasted_iota(jnp.int32, (planes, OVL), 0)
    acc = jnp.zeros((planes, 2 * rank), jnp.float32)
    ends = [slice((r + 1) * COLS - OVL, (r + 1) * COLS) for r in range(ROWS)]
    dark_ends = [dark[:, x].astype(jnp.float32) for x in ends]
    rows = []
    for c in range(CHUNKS):
        if c == CHUNKS - 1:
            small[0].wait()
            for t in range(tiles):
                limits[t] = jnp.full(limits.shape[1:], counts[t], jnp.int32)
        large[c].wait()
        rows.append(
            lax.dot_general(
                raw[c * chunk : (c + 1) * chunk].reshape(chunk * planes, pixels), weights,
                contract, preferred_element_type=jnp.float32,
            ).reshape(chunk, planes, 2 * rank)
        )
    for t in range(tiles):
        acc = acc + jnp.where(plane < counts[t], rows[t // chunk][t % chunk] - dark_rows, 0.0)
        for r in range(ROWS):
            value = raw[t, :, ends[r]].astype(jnp.float32)
            kept = jnp.where(wide_plane < counts[t], value, dark_ends[r])
            edges[t, :, r * OVL : (r + 1) * OVL] = kept.astype(jnp.bfloat16)
    pad = jnp.zeros((planes, LANES - 2 * rank), jnp.float32)
    rows = packed(jnp.concatenate([acc, pad], axis=1))
    out[...] = jnp.broadcast_to(rows[None], out.shape)


def pair_weights():
    row = lax.broadcasted_iota(jnp.int32, (WIDE, LANES), 0)
    col = lax.broadcasted_iota(jnp.int32, (WIDE, LANES), 1)
    hit = row // 2 == col
    up = (row.astype(jnp.float32) + 0.5) / OVL
    down = (WIDE - row.astype(jnp.float32) - 0.5) / OVL

    def of(scale):
        return jnp.where(hit, 0.25 * jnp.minimum(1.0, scale), 0.0).astype(jnp.bfloat16)

    return of(up), of(jnp.ones_like(up)), of(down)


def tail_weights():
    row = lax.broadcasted_iota(jnp.int32, (ROWS * OVL, LANES), 0) % OVL
    col = lax.broadcasted_iota(jnp.int32, (ROWS * OVL, LANES), 1) % HALF
    scale = jnp.minimum(1.0, (OVL - row.astype(jnp.float32) - 0.5) / OVL)
    return jnp.where(row // 2 == col, 0.25 * scale, 0.0).astype(jnp.bfloat16)


def block_cells(j, weight, raw, dark, inverse, limits, corrected):
    tiles, planes, _ = raw.shape
    plane = lax.broadcasted_iota(jnp.int32, (planes, WIDE), 0)
    acc = None
    for r in range(ROWS):
        x = slice(r * COLS + j * WIDE, r * COLS + (j + 1) * WIDE)
        scale = inverse[:, x]
        dark_f = dark[:, x].astype(jnp.float32)
        for t in range(tiles):
            value = (raw[t, :, x].astype(jnp.float32) - dark_f) * scale
            corrected[t, :, x] = jnp.where(plane < limits[t], value, 0.0).astype(jnp.bfloat16)
        part = jnp.dot(
            corrected[:, :, x].reshape(tiles * planes, WIDE), weight,
            preferred_element_type=jnp.float32,
        )
        acc = part if acc is None else acc + part
    return acc.astype(jnp.bfloat16).reshape(tiles, planes, LANES)


def fill_inverse(parts, basis, inverse):
    rank = basis.shape[0]
    terms = unpacked(jnp.sum(parts[...], axis=0))
    coef = (terms / pltpu.roll(terms, LANES - rank, 1))[:, :rank]
    high = coef.astype(jnp.bfloat16)
    rest = coef - high.astype(jnp.float32)
    middle = rest.astype(jnp.bfloat16)
    low = (rest - middle.astype(jnp.float32)).astype(jnp.bfloat16)
    coef3 = jnp.concatenate([high, middle, low], axis=1)
    base = basis[...]
    shade = jnp.dot(
        coef3, jnp.concatenate([base, base, base], axis=0), preferred_element_type=jnp.float32
    )
    inverse[...] = jnp.exp(-shade)


def store_tails(edges, dark, inverse, tails):
    tiles, planes, _ = edges.shape
    half = planes // 2
    ends = [slice((r + 1) * COLS - OVL, (r + 1) * COLS) for r in range(ROWS)]
    value = jnp.concatenate(
        [
            ((edges[:, :, r * OVL : (r + 1) * OVL].astype(jnp.float32)
              - dark[:, x].astype(jnp.float32)[None]) * inverse[:, x][None]).astype(jnp.bfloat16)
            for r, x in enumerate(ends)
        ],
        axis=2,
    )
    sums = jnp.dot(
        value.reshape(tiles * planes, ROWS * OVL), tail_weights(),
        preferred_element_type=jnp.float32,
    ).reshape(tiles, planes, LANES)
    left = lax.broadcasted_iota(jnp.int32, (half, LANES), 1) < HALF
    for t in range(tiles):
        tails[t] = jnp.where(left, sums[t, :half], sums[t, half:]).astype(jnp.bfloat16)


def correct_kernel(
    positions_h, parts, raw, dark, basis, edges, limits, corrected, cells_h,
    cells, tails, early, inverse, positions, sem,
):
    tiles, planes, _ = raw.shape
    half = planes // 2
    blocks = COLS // WIDE
    band_size = lax.axis_size(DEV) * tiles
    fetch = pltpu.make_async_copy(positions_h, positions, sem.at[blocks])
    fetch.start()
    own = (lax.axis_index(GRP) * lax.axis_size(DEV) + lax.axis_index(DEV)) * tiles
    before = jnp.maximum(own - tiles, 0)
    fill_inverse(parts, basis, inverse)
    store_tails(edges, dark, inverse, tails)
    first, inner, last = pair_weights()
    leaving = []

    def leave(x, slot):
        copy = pltpu.make_async_copy(cells.at[:, x, :], cells_h.at[:, x, :], sem.at[slot])
        copy.start()
        leaving.append(copy)

    for j in range(blocks):
        weight = first if j == 0 else last if j == blocks - 1 else inner
        pooled = block_cells(j, weight, raw, dark, inverse, limits, corrected)
        if j < EARLY:
            early[j] = pooled
            continue
        if j == EARLY:
            fetch.wait()
            bands = [positions[own + t] // band_size for t in range(tiles)]
            for t in range(tiles):
                cells[positions[before + t] // band_size, blocks * planes :, :] = tails[t]
                for i in range(EARLY):
                    cells[bands[t], i * planes : (i + 1) * planes, :] = early[i, t]
            leave(slice(blocks * planes, blocks * planes + half), 0)
            leave(slice(0, EARLY * planes), 1)
        for t in range(tiles):
            cells[bands[t], j * planes : (j + 1) * planes, :] = pooled[t]
        leave(slice(j * planes, (j + 1) * planes), j)
    for copy in leaving:
        copy.wait()


def flush_kernel(held, out_h, sem):
    copy = pltpu.make_async_copy(held, out_h, sem)
    copy.start()
    copy.wait()


def stitch_kernel(sources, arrived, out_h, out, sem):
    planes = out.shape[0]
    count = arrived.shape[0]
    blocks = COLS // 2 // LANES
    step = (COLS - OVL) // 2
    lane = lax.broadcasted_iota(jnp.int32, (planes, LANES), 1)
    left = lane < HALF

    def tile(source):
        return jnp.concatenate(
            [arrived[source, j * planes : (j + 1) * planes, :] for j in range(blocks)], axis=1
        ).astype(jnp.float32)

    spill = arrived[sources[count], blocks * planes :, :].astype(jnp.float32)
    spill = jnp.concatenate([spill, pltpu.roll(spill, HALF, 1)], axis=0)
    carry = jnp.where(left & (lax.axis_index(DEV) > 0), spill, 0.0)
    copies = []
    for j in range(0, count, 2):
        here = tile(sources[j])
        after = pltpu.roll(tile(sources[j + 1]), HALF, 1)
        edge = after[:, :LANES]
        width = here.shape[1]
        segment = jnp.concatenate(
            [
                here[:, :LANES] + carry,
                here[:, LANES : width - LANES],
                here[:, width - LANES :] + jnp.where(left, 0.0, edge),
                after[:, LANES:],
            ],
            axis=1,
        )
        x = slice(j * step, (j + 2) * step)
        out[:, x] = segment.astype(jnp.bfloat16)
        copy = pltpu.make_async_copy(out.at[:, x], out_h.at[:, x], sem.at[j // 2])
        copy.start()
        copies.append(copy)
        carry = jnp.where(left, edge, 0.0)
    for copy in copies:
        copy.wait()


SMEM = pl.BlockSpec(memory_space=pltpu.SMEM)
VMEM = pl.BlockSpec(memory_space=pltpu.VMEM)
HBM = pl.BlockSpec(memory_space=pltpu.HBM)
LIMIT = pltpu.CompilerParams(vmem_limit_bytes=16 << 20)


def in_vmem(value):
    return pltpu.with_memory_space_constraint(value, pltpu.VMEM)


def in_hbm(value):
    return pltpu.with_memory_space_constraint(value, pltpu.HBM)


def exchanged(copies, axes):
    return lax.all_to_all(copies, axes, split_axis=0, concat_axis=0, tiled=True)


def sources_of(positions, column, groups, columns, tiles):
    layout = positions.reshape(groups, columns, tiles)
    column_tiles = lax.dynamic_index_in_dim(layout, column, 1, False)
    arrives = column_tiles // (columns * tiles) == lax.axis_index(GRP)
    slot_of = jnp.sum(jnp.where(arrives, column_tiles % tiles, 0), axis=1)
    slots = jnp.arange(tiles, dtype=jnp.int32)
    ids = jnp.arange(groups, dtype=jnp.int32)
    return jnp.sum(jnp.where(slot_of[None, :] == slots[:, None], ids[None, :], 0), axis=1)


def per_device(raw, dark, basis, counts, positions):
    tiles, planes, _ = raw.shape
    groups = lax.axis_size(GRP)
    columns = lax.axis_size(DEV)
    width = COLS // 2
    span = tiles * (COLS - OVL) // 2
    height = width // LANES * planes + planes // 2
    first, second = lax.axis_size(FIRST), lax.axis_size(SECOND)
    terms, raw_v, dark_v, basis_v, edges, limits = pl.pallas_call(
        terms_kernel,
        out_shape=(
            jax.ShapeDtypeStruct((first, planes // SUBLANES, LANES), jnp.float32),
            pltpu.VMEM(raw.shape, jnp.bfloat16),
            pltpu.VMEM(dark.shape, jnp.bfloat16),
            pltpu.VMEM(basis.shape, jnp.bfloat16),
            jax.ShapeDtypeStruct((tiles, planes, ROWS * OVL), jnp.bfloat16),
            pltpu.VMEM((tiles, planes, WIDE), jnp.int32),
        ),
        in_specs=[HBM, HBM, HBM, HBM],
        out_specs=(VMEM,) * 6,
        scratch_shapes=[
            pltpu.SMEM((tiles,), jnp.int32),
            pltpu.SemaphoreType.DMA((CHUNKS + 3,)),
        ],
        compiler_params=LIMIT,
        name="terms",
    )(in_hbm(counts), in_hbm(raw), in_hbm(dark), in_hbm(basis))
    column_sums = exchanged(terms, FIRST)
    edges = lax.ppermute(edges, DEV, [(d, d + 1) for d in range(columns - 1)])
    once = jnp.sum(column_sums, axis=0)
    parts = exchanged(jnp.broadcast_to(once[None], (second, *once.shape)), SECOND)
    positions_late, parts = lax.optimization_barrier((positions, parts))
    here_dev = lax.axis_index(DEV)
    own_sources = sources_of(positions_late, here_dev, groups, columns, tiles)
    left_dev = jnp.maximum(here_dev - 1, 0)
    left_sources = sources_of(positions_late, left_dev, groups, columns, tiles)
    sources = jnp.concatenate([own_sources, left_sources[tiles - 1 :]])
    corrected, outgoing = pl.pallas_call(
        correct_kernel,
        out_shape=(
            pltpu.VMEM(raw.shape, jnp.bfloat16),
            jax.ShapeDtypeStruct((groups, height, LANES), jnp.bfloat16),
        ),
        in_specs=[HBM] + [VMEM] * 6,
        out_specs=(VMEM, HBM),
        scratch_shapes=[
            pltpu.VMEM((groups, height, LANES), jnp.bfloat16),
            pltpu.VMEM((tiles, planes // 2, LANES), jnp.bfloat16),
            pltpu.VMEM((EARLY, tiles, planes, LANES), jnp.bfloat16),
            pltpu.VMEM(dark.shape, jnp.float32),
            pltpu.SMEM(positions.shape, jnp.int32),
            pltpu.SemaphoreType.DMA((COLS // WIDE + 1,)),
        ],
        input_output_aliases={2: 0},
        compiler_params=LIMIT,
        name="correct",
    )(
        in_hbm(positions), in_vmem(parts), in_vmem(raw_v), in_vmem(dark_v), in_vmem(basis_v),
        in_vmem(edges), in_vmem(limits),
    )
    arrived = exchanged(outgoing, GRP)
    flushed = pl.pallas_call(
        flush_kernel,
        out_shape=jax.ShapeDtypeStruct(raw.shape, jnp.bfloat16),
        in_specs=[VMEM],
        out_specs=HBM,
        scratch_shapes=[pltpu.SemaphoreType.DMA],
        compiler_params=LIMIT,
        name="flush",
    )(in_vmem(corrected))
    pooled = pl.pallas_call(
        stitch_kernel,
        out_shape=jax.ShapeDtypeStruct((planes, span), jnp.bfloat16),
        in_specs=[SMEM, VMEM],
        out_specs=HBM,
        scratch_shapes=[
            pltpu.VMEM((planes, span), jnp.bfloat16),
            pltpu.SemaphoreType.DMA((tiles // 2,)),
        ],
        compiler_params=LIMIT,
        name="stitch",
    )(sources, in_vmem(arrived))
    return flushed, pooled.reshape(1, planes, ROWS // 2, span)


def solution(mesh):
    split = Mesh(mesh.devices.reshape(4, 4, 2, 8, 2), GRP_DEV)
    placed = (P(GRP_DEV, None, None), P(), P(), P(GRP_DEV), P())
    return jax.shard_map(
        per_device,
        mesh=split,
        in_specs=placed,
        out_specs=(P(GRP_DEV, None, None), P(GRP, None, None, DEV)),
        check_vma=False,
    )
```

```python
import jax
import jax.numpy as jnp
from jax import lax
from jax.experimental import pallas as pl
from jax.experimental.pallas import tpu as pltpu
from jax.sharding import Mesh
from jax.sharding import PartitionSpec as P

ROWS = 2
COLS = 2048
OVL = 128
GRP = ("grp_0", "grp_1")
DEV = ("dev_0", "dev_1", "dev_2")
GRP_DEV = GRP + DEV
FIRST = ("dev_1", "dev_2")
SECOND = ("grp_0", "grp_1", "dev_0")
LANES = 128
WIDE = 256
HALF = LANES // 2
SUBLANES = 8
PARTS = 16
EARLY = 3


def packed(rows):
    planes = rows.shape[0]
    lane = lax.broadcasted_iota(jnp.int32, (planes, LANES), 1)
    plane = lax.broadcasted_iota(jnp.int32, (planes, LANES), 0)
    wide = jnp.where(lane < PARTS, rows, 0.0)
    for shift in (PARTS, 2 * PARTS, 4 * PARTS):
        wide = wide + pltpu.roll(wide, shift, 1)
    chosen = jnp.where(lane // PARTS == plane % SUBLANES, wide, 0.0)
    return jnp.sum(chosen.reshape(planes // SUBLANES, SUBLANES, LANES), axis=1)


def unpacked(rows):
    count = rows.shape[0]
    planes = count * SUBLANES
    lane = lax.broadcasted_iota(jnp.int32, (planes, LANES), 1)
    plane = lax.broadcasted_iota(jnp.int32, (planes, LANES), 0)
    spread = jnp.broadcast_to(rows[:, None, :], (count, SUBLANES, LANES)).reshape(planes, LANES)
    wide = jnp.where(lane // PARTS == plane % SUBLANES, spread, 0.0)
    for shift in (PARTS, 2 * PARTS, 4 * PARTS):
        wide = wide + pltpu.roll(wide, shift, 1)
    return wide


def chunks_of(pixels):
    most = 3 * pixels // 4
    return [slice(0, most), slice(most, pixels)]


def terms_kernel(
    counts_h, raw_h, dark_h, basis_h, out_h, raw, dark, basis, edges, out, counts, sem
):
    tiles, planes, pixels = raw_h.shape
    rank = basis.shape[0]
    chunks = chunks_of(pixels)
    count = len(chunks)
    small = [
        pltpu.make_async_copy(counts_h, counts, sem.at[count]),
        pltpu.make_async_copy(basis_h, basis, sem.at[count + 1]),
        pltpu.make_async_copy(dark_h, raw.at[tiles], sem.at[count + 2]),
        pltpu.make_async_copy(dark_h, dark, sem.at[count + 4]),
    ]
    large = [
        pltpu.make_async_copy(raw_h.at[:, :, x], raw.at[pl.ds(0, tiles), :, x], sem.at[c])
        for c, x in enumerate(chunks)
    ]
    for copy in small + large:
        copy.start()
    plane = lax.broadcasted_iota(jnp.int32, (planes, 2 * rank), 0)
    wide_plane = lax.broadcasted_iota(jnp.int32, (planes, WIDE), 0)

    def mask(chunk):
        for t in range(tiles):
            alive = wide_plane < counts[t]
            for start in range(chunk.start, chunk.stop, WIDE):
                x = slice(start, start + WIDE)
                raw[t, :, x] = jnp.where(alive, raw[t, :, x], dark[:, x])

    for copy in small:
        copy.wait()
    rows = None
    for c, x in enumerate(chunks):
        fill = jnp.ones((rank, x.stop - x.start), jnp.bfloat16)
        weights = jnp.concatenate([basis[:, x], fill], axis=0)
        large[c].wait()
        part = lax.dot_general(
            raw[:, :, x].reshape((tiles + 1) * planes, x.stop - x.start), weights,
            (((1,), (1,)), ((), ())), preferred_element_type=jnp.float32,
        )
        rows = part if rows is None else rows + part
    rows = rows.reshape(tiles + 1, planes, 2 * rank)
    acc = jnp.zeros((planes, 2 * rank), jnp.float32)
    for t in range(tiles):
        acc = acc + jnp.where(plane < counts[t], rows[t] - rows[tiles], 0.0)
    pad = jnp.zeros((planes, LANES - 2 * rank), jnp.float32)
    out[...] = jnp.broadcast_to(packed(jnp.concatenate([acc, pad], axis=1))[None], out.shape)
    leave = pltpu.make_async_copy(out, out_h, sem.at[count + 3])
    leave.start()
    mask(slice(0, pixels))
    for t in range(tiles):
        for r in range(ROWS):
            end = (r + 1) * COLS
            edges[t, :, r * OVL : (r + 1) * OVL] = raw[t, :, end - OVL : end]
    leave.wait()


def pair_weights():
    row = lax.broadcasted_iota(jnp.int32, (WIDE, LANES), 0)
    col = lax.broadcasted_iota(jnp.int32, (WIDE, LANES), 1)
    hit = row // 2 == col
    up = (row.astype(jnp.float32) + 0.5) / OVL
    down = (WIDE - row.astype(jnp.float32) - 0.5) / OVL

    def of(scale):
        return jnp.where(hit, 0.25 * jnp.minimum(1.0, scale), 0.0).astype(jnp.bfloat16)

    return of(up), of(jnp.ones_like(up)), of(down)


def tail_weights():
    row = lax.broadcasted_iota(jnp.int32, (ROWS * OVL, LANES), 0) % OVL
    col = lax.broadcasted_iota(jnp.int32, (ROWS * OVL, LANES), 1) % HALF
    scale = jnp.minimum(1.0, (OVL - row.astype(jnp.float32) - 0.5) / OVL)
    return jnp.where(row // 2 == col, 0.25 * scale, 0.0).astype(jnp.bfloat16)


def block_cells(j, weight, raw, dark, inverse, corrected):
    tiles, planes = raw.shape[0] - 1, raw.shape[1]
    acc = None
    for r in range(ROWS):
        x = slice(r * COLS + j * WIDE, r * COLS + (j + 1) * WIDE)
        scale = inverse[:, x]
        dark_f = dark[:, x].astype(jnp.float32)
        for t in range(tiles):
            value = (raw[t, :, x].astype(jnp.float32) - dark_f) * scale
            corrected[t, :, x] = value.astype(jnp.bfloat16)
        part = jnp.dot(
            corrected[:tiles, :, x].reshape(tiles * planes, WIDE), weight,
            preferred_element_type=jnp.float32,
        )
        acc = part if acc is None else acc + part
    return acc.astype(jnp.bfloat16).reshape(tiles, planes, LANES)


def fill_inverse(parts, basis, inverse):
    rank = basis.shape[0]
    terms = unpacked(jnp.sum(parts[...], axis=0))
    coef = (terms / pltpu.roll(terms, LANES - rank, 1))[:, :rank]
    high = coef.astype(jnp.bfloat16)
    rest = coef - high.astype(jnp.float32)
    middle = rest.astype(jnp.bfloat16)
    low = (rest - middle.astype(jnp.float32)).astype(jnp.bfloat16)
    coef3 = jnp.concatenate([high, middle, low], axis=1)
    base = basis[...]
    shade = jnp.dot(
        coef3, jnp.concatenate([base, base, base], axis=0), preferred_element_type=jnp.float32
    )
    inverse[...] = jnp.exp(-shade)


def store_tails(edges, dark, inverse, tails):
    tiles, planes, _ = edges.shape
    half = planes // 2
    ends = [slice((r + 1) * COLS - OVL, (r + 1) * COLS) for r in range(ROWS)]
    value = jnp.concatenate(
        [
            ((edges[:, :, r * OVL : (r + 1) * OVL].astype(jnp.float32)
              - dark[:, x].astype(jnp.float32)[None]) * inverse[:, x][None]).astype(jnp.bfloat16)
            for r, x in enumerate(ends)
        ],
        axis=2,
    )
    sums = jnp.dot(
        value.reshape(tiles * planes, ROWS * OVL), tail_weights(),
        preferred_element_type=jnp.float32,
    ).reshape(tiles, planes, LANES)
    left = lax.broadcasted_iota(jnp.int32, (half, LANES), 1) < HALF
    for t in range(tiles):
        tails[t] = jnp.where(left, sums[t, :half], sums[t, half:]).astype(jnp.bfloat16)


def correct_kernel(
    positions_h, parts, raw, dark, basis, edges, corrected, cells_h,
    cells, tails, early, inverse, positions, sem,
):
    tiles, planes, _ = edges.shape
    half = planes // 2
    blocks = COLS // WIDE
    band_size = lax.axis_size(DEV) * tiles
    fetch = pltpu.make_async_copy(positions_h, positions, sem.at[blocks])
    fetch.start()
    own = (lax.axis_index(GRP) * lax.axis_size(DEV) + lax.axis_index(DEV)) * tiles
    before = jnp.maximum(own - tiles, 0)
    fill_inverse(parts, basis, inverse)
    store_tails(edges, dark, inverse, tails)
    first, inner, last = pair_weights()
    leaving = []

    def leave(x, slot):
        copy = pltpu.make_async_copy(cells.at[:, x, :], cells_h.at[:, x, :], sem.at[slot])
        copy.start()
        leaving.append(copy)

    for j in range(blocks):
        weight = first if j == 0 else last if j == blocks - 1 else inner
        pooled = block_cells(j, weight, raw, dark, inverse, corrected)
        if j < EARLY:
            early[j] = pooled
            continue
        if j == EARLY:
            fetch.wait()
            bands = [positions[own + t] // band_size for t in range(tiles)]
            for t in range(tiles):
                cells[positions[before + t] // band_size, blocks * planes :, :] = tails[t]
                for i in range(EARLY):
                    cells[bands[t], i * planes : (i + 1) * planes, :] = early[i, t]
            leave(slice(blocks * planes, blocks * planes + half), 0)
            leave(slice(0, EARLY * planes), 1)
        for t in range(tiles):
            cells[bands[t], j * planes : (j + 1) * planes, :] = pooled[t]
        leave(slice(j * planes, (j + 1) * planes), j)
    for copy in leaving:
        copy.wait()


def flush_kernel(held, out_h, sem):
    copy = pltpu.make_async_copy(held.at[pl.ds(0, out_h.shape[0])], out_h, sem)
    copy.start()
    copy.wait()


def stitch_kernel(sources, arrived, out_h, out, sem):
    planes = out.shape[0]
    count = arrived.shape[0]
    blocks = COLS // 2 // LANES
    step = (COLS - OVL) // 2
    lane = lax.broadcasted_iota(jnp.int32, (planes, LANES), 1)
    left = lane < HALF

    def tile(source):
        return jnp.concatenate(
            [arrived[source, j * planes : (j + 1) * planes, :] for j in range(blocks)], axis=1
        ).astype(jnp.float32)

    spill = arrived[sources[count], blocks * planes :, :].astype(jnp.float32)
    spill = jnp.concatenate([spill, pltpu.roll(spill, HALF, 1)], axis=0)
    carry = jnp.where(left & (lax.axis_index(DEV) > 0), spill, 0.0)
    copies = []
    for j in range(0, count, 2):
        here = tile(sources[j])
        after = pltpu.roll(tile(sources[j + 1]), HALF, 1)
        edge = after[:, :LANES]
        width = here.shape[1]
        segment = jnp.concatenate(
            [
                here[:, :LANES] + carry,
                here[:, LANES : width - LANES],
                here[:, width - LANES :] + jnp.where(left, 0.0, edge),
                after[:, LANES:],
            ],
            axis=1,
        )
        x = slice(j * step, (j + 2) * step)
        out[:, x] = segment.astype(jnp.bfloat16)
        copy = pltpu.make_async_copy(out.at[:, x], out_h.at[:, x], sem.at[j // 2])
        copy.start()
        copies.append(copy)
        carry = jnp.where(left, edge, 0.0)
    for copy in copies:
        copy.wait()


SMEM = pl.BlockSpec(memory_space=pltpu.SMEM)
VMEM = pl.BlockSpec(memory_space=pltpu.VMEM)
HBM = pl.BlockSpec(memory_space=pltpu.HBM)
LIMIT = pltpu.CompilerParams(vmem_limit_bytes=16 << 20)


def in_vmem(value):
    return pltpu.with_memory_space_constraint(value, pltpu.VMEM)


def in_hbm(value):
    return pltpu.with_memory_space_constraint(value, pltpu.HBM)


def exchanged(copies, axes):
    return lax.all_to_all(copies, axes, split_axis=0, concat_axis=0, tiled=True)


def sources_of(positions, column, groups, columns, tiles):
    layout = positions.reshape(groups, columns, tiles)
    column_tiles = lax.dynamic_index_in_dim(layout, column, 1, False)
    arrives = column_tiles // (columns * tiles) == lax.axis_index(GRP)
    slot_of = jnp.sum(jnp.where(arrives, column_tiles % tiles, 0), axis=1)
    slots = jnp.arange(tiles, dtype=jnp.int32)
    ids = jnp.arange(groups, dtype=jnp.int32)
    return jnp.sum(jnp.where(slot_of[None, :] == slots[:, None], ids[None, :], 0), axis=1)


def per_device(raw, dark, basis, counts, positions):
    tiles, planes, pixels = raw.shape
    groups = lax.axis_size(GRP)
    columns = lax.axis_size(DEV)
    width = COLS // 2
    span = tiles * (COLS - OVL) // 2
    height = width // LANES * planes + planes // 2
    first, second = lax.axis_size(FIRST), lax.axis_size(SECOND)
    terms, raw_v, dark_v, basis_v, edges = pl.pallas_call(
        terms_kernel,
        out_shape=(
            jax.ShapeDtypeStruct((first, planes // SUBLANES, LANES), jnp.float32),
            pltpu.VMEM((tiles + 1, planes, pixels), jnp.bfloat16),
            pltpu.VMEM(dark.shape, jnp.bfloat16),
            pltpu.VMEM(basis.shape, jnp.bfloat16),
            jax.ShapeDtypeStruct((tiles, planes, ROWS * OVL), jnp.bfloat16),
        ),
        in_specs=[HBM, HBM, HBM, HBM],
        out_specs=(HBM,) + (VMEM,) * 4,
        scratch_shapes=[
            pltpu.VMEM((first, planes // SUBLANES, LANES), jnp.float32),
            pltpu.SMEM((tiles,), jnp.int32),
            pltpu.SemaphoreType.DMA((len(chunks_of(pixels)) + 5,)),
        ],
        compiler_params=LIMIT,
        name="terms",
    )(in_hbm(counts), in_hbm(raw), in_hbm(dark), in_hbm(basis))
    column_sums = exchanged(terms, FIRST)
    edges = lax.ppermute(edges, DEV, [(d, d + 1) for d in range(columns - 1)])
    once = jnp.sum(column_sums, axis=0)
    parts = exchanged(jnp.broadcast_to(once[None], (second, *once.shape)), SECOND)
    positions_late, parts = lax.optimization_barrier((positions, parts))
    here_dev = lax.axis_index(DEV)
    own_sources = sources_of(positions_late, here_dev, groups, columns, tiles)
    left_dev = jnp.maximum(here_dev - 1, 0)
    left_sources = sources_of(positions_late, left_dev, groups, columns, tiles)
    sources = jnp.concatenate([own_sources, left_sources[tiles - 1 :]])
    corrected, outgoing = pl.pallas_call(
        correct_kernel,
        out_shape=(
            pltpu.VMEM(raw_v.shape, jnp.bfloat16),
            jax.ShapeDtypeStruct((groups, height, LANES), jnp.bfloat16),
        ),
        in_specs=[HBM] + [VMEM] * 5,
        out_specs=(VMEM, HBM),
        scratch_shapes=[
            pltpu.VMEM((groups, height, LANES), jnp.bfloat16),
            pltpu.VMEM((tiles, planes // 2, LANES), jnp.bfloat16),
            pltpu.VMEM((EARLY, tiles, planes, LANES), jnp.bfloat16),
            pltpu.VMEM(dark.shape, jnp.float32),
            pltpu.SMEM(positions.shape, jnp.int32),
            pltpu.SemaphoreType.DMA((COLS // WIDE + 1,)),
        ],
        input_output_aliases={2: 0},
        compiler_params=LIMIT,
        name="correct",
    )(
        in_hbm(positions), in_vmem(parts), in_vmem(raw_v), in_vmem(dark_v), in_vmem(basis_v),
        in_vmem(edges),
    )
    arrived = exchanged(outgoing, GRP)
    flushed = pl.pallas_call(
        flush_kernel,
        out_shape=jax.ShapeDtypeStruct(raw.shape, jnp.bfloat16),
        in_specs=[VMEM],
        out_specs=HBM,
        scratch_shapes=[pltpu.SemaphoreType.DMA],
        compiler_params=LIMIT,
        name="flush",
    )(in_vmem(corrected))
    pooled = pl.pallas_call(
        stitch_kernel,
        out_shape=jax.ShapeDtypeStruct((planes, span), jnp.bfloat16),
        in_specs=[SMEM, VMEM],
        out_specs=HBM,
        scratch_shapes=[
            pltpu.VMEM((planes, span), jnp.bfloat16),
            pltpu.SemaphoreType.DMA((tiles // 2,)),
        ],
        compiler_params=LIMIT,
        name="stitch",
    )(sources, in_vmem(arrived))
    return flushed, pooled.reshape(1, planes, ROWS // 2, span)


def solution(mesh):
    split = Mesh(mesh.devices.reshape(4, 4, 2, 8, 2), GRP_DEV)
    placed = (P(GRP_DEV, None, None), P(), P(), P(GRP_DEV), P())
    return jax.shard_map(
        per_device,
        mesh=split,
        in_specs=placed,
        out_specs=(P(GRP_DEV, None, None), P(GRP, None, None, DEV)),
        check_vma=False,
    )
```
